32 devices in a mesh: row: 4 (over z), col: 8 (over y, x, core).
Axes of the slice: x: 2, y: 2, z: 4, core: 2. Of those that a mesh axis runs over, the one named last changes fastest.
Arguments:
- gram: bfloat16 [2, 4, 384, 1, 8, 384], P(None, 'row', None, None, 'col'), may hold values from -1 to 20, as said below
Outputs:
- swept: float32 [2, 4, 384, 1, 8, 384], P(None, 'row', None, None, 'col')
The draws below stay inside these ranges and needn't reach their ends.
Inputs may be any that keep to these rules, and one draw needn't show every extreme that they name: gram is symmetric and positive definite.
All inputs are finite; a program needn't handle non-finite values.
Results may differ from the reference program's by a relative error of at most 0.0003.
Values sent between devices are 32-bit elements; how exact they have to be, the bound alone decides.
No kernel may reach another device: no remote copies, remote signals or barrier semaphores. Data moves between devices by JAX's collectives and lax.ppermute only.
A program may use at most 64 MiB of HBM per device.

```python
import math
import jax
import jax.numpy as jnp
from jax import lax

TB = 384
LC = 1
PANELS = 2
LR = 2
ORDER = 3072
N_ROW = 4
N_COL = 8


def draw_gram(key, part):
    key_noise, key_diagonal = jax.random.split(key, 2)
    noise = jax.random.truncated_normal(key_noise, -4.0, 4.0, (ORDER, ORDER), jnp.float32)
    spread = 1.2 / math.sqrt(2.0 * ORDER)
    symmetric = (noise + noise.T) * spread
    diagonal = jax.random.uniform(key_diagonal, (ORDER,), jnp.float32, 3.0, 6.0)
    matrix = symmetric + jnp.diag(diagonal)
    return matrix.astype(jnp.bfloat16).reshape(LR, N_ROW, TB, LC, N_COL, TB)


def setup_inputs(seed: int = 0) -> dict:
    arg_keys = jax.random.split(jax.random.key(seed), 2)
    gram = draw_gram(jax.random.fold_in(arg_keys[1], 71), 0)
    return {"gram": gram}


def reference(gram):
    matrix = gram.astype(jnp.float32).reshape(ORDER, ORDER)
    identity = jnp.eye(TB, dtype=jnp.float32)
    for number in range(PANELS):
        lower = number * TB
        upper = lower + TB
        factor = jnp.linalg.cholesky(matrix[lower:upper, lower:upper])
        right_side = matrix[lower:upper].at[:, lower:upper].set(identity)
        solved = jax.scipy.linalg.cho_solve((factor, True), right_side)
        shifted = solved.at[:, lower:upper].add(identity)

        def sweep_rows(index, current):
            start = (index * TB).astype(jnp.int32)
            rows = lax.dynamic_slice(current, (start, jnp.int32(0)), (TB, ORDER))
            fresh = rows - jnp.dot(rows[:, lower:upper].astype(jnp.float32), shifted.astype(jnp.float32), precision=lax.Precision.HIGHEST, preferred_element_type=jnp.float32)
            return lax.dynamic_update_slice(current, fresh, (start, jnp.int32(0)))
        matrix = lax.fori_loop(0, ORDER // TB, sweep_rows, matrix)
        matrix = matrix.at[lower:upper].set(solved)
    return matrix.reshape(gram.shape)
```

```python
import functools

import jax
import jax.numpy as jnp
from jax import lax
from jax.experimental import pallas as pl
from jax.experimental.pallas import tpu as pltpu
from jax.sharding import PartitionSpec as P

LEAF = 16
LANES = 128


def split(value):
    high = value.astype(jnp.bfloat16)
    low = (value - high.astype(jnp.float32)).astype(jnp.bfloat16)
    return high, low


def dot3(left, right):
    dot = functools.partial(jnp.dot, preferred_element_type=jnp.float32)
    return dot(left[0], right[0]) + dot(left[0], right[1]) + dot(left[1], right[0])


def inverse_kernel(flag_ref, a_ref, o_ref, right_ref):
    order = a_ref.shape[0]
    blocks = order // LANES
    groups = LANES // LEAF

    @pl.when(flag_ref[0] != 0)
    def _():
        o_ref[...] = a_ref[...]
        right_ref[...] = jnp.zeros_like(right_ref)
        rows_leaf = lax.broadcasted_iota(jnp.int32, (LEAF, LANES), 0)
        rows_wide = lax.broadcasted_iota(jnp.int32, (LEAF, order), 0)
        lanes_wide = lax.broadcasted_iota(jnp.int32, (LEAF, order), 1)
        lanes_left = lax.broadcasted_iota(jnp.int32, (order, LANES), 1)
        lanes_full = lax.broadcasted_iota(jnp.int32, (order, order), 1)
        nothing = jnp.zeros((LEAF, order), jnp.bfloat16)

        def block(number, _):
            base = pl.multiple_of(number * LANES, LANES)
            for group in range(groups):
                lower = group * LEAF
                rows = pl.ds(pl.multiple_of(base + lower, LEAF), LEAF)
                tile = o_ref[rows, pl.ds(base, LANES)]
                columns = [
                    jnp.broadcast_to(tile[:, lower + k : lower + k + 1], (LEAF, LANES))
                    for k in range(LEAF)
                ]
                wide = o_ref[rows, :]
                here = lanes_wide - (base + lower)
                unit = jnp.where(here == rows_wide, 1.0, 0.0)
                wide = jnp.where((here >= 0) & (here < LEAF), unit, wide)
                for k in range(LEAF):
                    pivot = columns[k][k : k + 1, :]
                    inverted = 1.0 / pivot
                    factor = jnp.where(rows_leaf == k, pivot - 1.0, columns[k])
                    for later in range(k + 1, LEAF):
                        row = columns[later][k : k + 1, :] * inverted
                        columns[later] = columns[later] - factor * row
                    parts = []
                    for part in range(order // LANES):
                        piece = wide[:, part * LANES : (part + 1) * LANES]
                        parts.append(piece - factor * (piece[k : k + 1, :] * inverted))
                    wide = jnp.concatenate(parts, axis=1)
                left = o_ref[:, pl.ds(base, LANES)]
                inside = (lanes_left >= lower) & (lanes_left < lower + LEAF)
                left = jnp.where(inside, left, 0.0)
                high, low = split(wide)
                right_ref[0, lower : lower + LEAF, :] = high
                right_ref[1, lower : lower + LEAF, :] = low
                if group:
                    right_ref[0, lower - LEAF : lower, :] = nothing
                    right_ref[1, lower - LEAF : lower, :] = nothing
                change = dot3(split(left), (right_ref[0], right_ref[1]))
                there = lanes_full - (base + lower)
                old = jnp.where((there >= 0) & (there < LEAF), 0.0, o_ref[...])
                o_ref[...] = old - change
                o_ref[rows, :] = wide
            right_ref[0, LANES - LEAF : LANES, :] = nothing
            right_ref[1, LANES - LEAF : LANES, :] = nothing
            return 0

        lax.fori_loop(0, blocks, block, 0)


def inverse(flag, matrix):
    return pl.pallas_call(
        inverse_kernel,
        out_shape=jax.ShapeDtypeStruct(matrix.shape, jnp.float32),
        in_specs=[
            pl.BlockSpec(memory_space=pltpu.SMEM),
            pl.BlockSpec(memory_space=pltpu.VMEM),
        ],
        out_specs=pl.BlockSpec(memory_space=pltpu.VMEM),
        scratch_shapes=[pltpu.VMEM((2, LANES, matrix.shape[1]), jnp.bfloat16)],
        name="inverse",
    )(flag, matrix)


def multiply(left, right, contract=(1, 0)):
    dims = (((contract[0],), (contract[1],)), ((), ()))
    return lax.dot_general(
        left, right, dims, precision=lax.Precision.HIGH, preferred_element_type=jnp.float32
    )


def on_device(gram):
    row_count = lax.axis_size("row")
    col_count = lax.axis_size("col")
    here_row = lax.axis_index("row")
    here_col = lax.axis_index("col")
    breadth = gram.shape[2]
    mine = gram.astype(jnp.float32).reshape(gram.shape[0] * breadth, breadth)
    first = mine[:breadth]
    odd = here_col % 2 == 1
    pair = here_col // 2
    steps = (col_count // 2).bit_length() - 1
    root = 1

    def send(value, pairs):
        lines = [(a[0] * col_count + a[1], b[0] * col_count + b[1]) for a, b in pairs]
        return lax.ppermute(value, ("row", "col"), lines)

    def swap(value):
        pairs = [((r, c), (r, c ^ 1)) for r in range(row_count) for c in range(col_count)]
        return send(value, pairs)

    def along_row(value, which):
        held = value
        for step in range(steps):
            pairs = []
            takes = jnp.zeros((), jnp.bool_)
            for parity in range(2):
                done = list(range(step)) if parity == 0 else list(range(steps - step, steps))
                bit = step if parity == 0 else steps - 1 - step
                targets = []
                for number in range(col_count // 2):
                    if all(number >> b & 1 == 0 for b in range(steps) if b not in done):
                        target = number | 1 << bit
                        targets.append(target)
                        for r in which:
                            pairs.append(((r, 2 * number + parity), (r, 2 * target + parity)))
                for target in targets:
                    takes = takes | (here_col == 2 * target + parity)
            got = send(held, pairs)
            held = jnp.where(takes, got, held)
        return held

    def along_column(value):
        held = value
        for r in range(root, 0, -1):
            got = send(held, [((r, c), (r - 1, c)) for c in range(col_count)])
            held = jnp.where(here_row == r - 1, got, held)
        for r in range(root, row_count - 1):
            got = send(held, [((r, c), (r + 1, c)) for c in range(col_count)])
            held = jnp.where(here_row == r + 1, got, held)
        return held

    sibling = swap(mine)
    down = send(first, [((0, c), (1, c)) for c in range(col_count)])
    up = send(first, [((1, c), (0, c)) for c in range(col_count)])
    top = jnp.where(here_row == 0, first, down)
    bottom = jnp.where(here_row == 1, first, up)
    passing = bottom
    for step in range(row_count - 2 + 1):
        pairs = []
        for r in range(1, row_count - 1):
            if 0 <= step - (r - 1) < 2:
                pairs += [((r, c), (r + 1, c)) for c in range(col_count)]
        got = send(passing, pairs)
        for r in range(2, row_count):
            if step - (r - 2) == 0:
                bottom = jnp.where(here_row == r, got, bottom)
            if step - (r - 2) == 1:
                top = jnp.where(here_row == r, got, top)
        passing = jnp.where(here_row == 1, top, got)

    lefts = along_row(mine, range(row_count))
    lefts_sibling = swap(lefts)
    left0 = jnp.where(odd, lefts_sibling, lefts)
    left1 = jnp.where(odd, lefts, lefts_sibling)

    at_root = (here_row == root) & (pair == 0)
    flag = at_root.astype(jnp.int32).reshape(1)
    a11 = jnp.where(odd, first, sibling[:breadth])
    a10 = jnp.where(odd, sibling[:breadth], first)
    down_sibling = swap(down)
    a00 = jnp.where(odd, down_sibling, down)
    n = inverse(flag, a11)
    g = multiply(n, a10)
    schur = a00 - multiply(a10, g, (0, 0))
    s = inverse(flag, schur)

    ng = along_column(along_row(jnp.where(odd, g, n), [root]))
    ng_sibling = swap(ng)
    n = jnp.where(odd, ng_sibling, ng)
    g = jnp.where(odd, ng, ng_sibling)
    half = breadth // 2
    s_half = along_column(along_row(jnp.where(odd, s[half:], s[:half]), [root]))
    s_sibling = swap(s_half)
    s = jnp.concatenate(
        [jnp.where(odd, s_sibling, s_half), jnp.where(odd, s_half, s_sibling)], axis=0
    )

    identity = jnp.eye(breadth, dtype=jnp.float32)
    pivotal = here_col < 2
    r0 = jnp.where(pivotal, jnp.where(here_col == 0, identity, 0.0), top)
    r1 = jnp.where(pivotal, jnp.where(here_col == 1, identity, 0.0), bottom)
    y0 = r0 - multiply(g, r1, (0, 0))
    y1 = multiply(n, r1)
    base = jnp.where(pivotal, 0.0, mine) - multiply(left1, y1)
    h = left0 - multiply(left1, g)
    w0 = multiply(s, y0)
    w1 = y1 - multiply(g, w0)
    out = base - multiply(h, w0)
    kept = jnp.where(here_row == 0, w0, jnp.where(here_row == 1, w1, out[:breadth]))
    out = jnp.concatenate([kept, out[breadth:]], axis=0)
    return out.reshape(gram.shape)


def solution(mesh):
    placed = (P(None, "row", None, None, "col", None),)
    return jax.shard_map(
        on_device,
        mesh=mesh,
        in_specs=placed,
        out_specs=P(None, "row", None, None, "col", None),
        check_vma=False,
    )
```

```python
import jax
import jax.numpy as jnp
from jax import lax
from jax.experimental import pallas as pl
from jax.experimental.pallas import tpu as pltpu
from jax.sharding import PartitionSpec as P


LEAF = 16
LANES = 128


def split(value):
    high = value.astype(jnp.bfloat16).astype(jnp.float32)
    rest = value - high
    middle = rest.astype(jnp.bfloat16).astype(jnp.float32)
    return high, middle, (rest - middle).astype(jnp.bfloat16).astype(jnp.float32)


def invert(ref, left_ref):
    order = ref.shape[0]
    blocks = order // LANES
    groups = LANES // LEAF
    rows_leaf = lax.broadcasted_iota(jnp.int32, (LEAF, LANES), 0)
    rows_wide = lax.broadcasted_iota(jnp.int32, (LEAF, order), 0)
    lanes_wide = lax.broadcasted_iota(jnp.int32, (LEAF, order), 1)
    lanes_left = lax.broadcasted_iota(jnp.int32, (order, LANES), 1)
    nothing = jnp.zeros((LEAF, order), jnp.bfloat16)

    def block(number, _):
        base = pl.multiple_of(number * LANES, LANES)
        lanes = pl.ds(base, LANES)
        wide = ref[pl.ds(base, LEAF), :]
        tile = ref[pl.ds(base, LEAF), lanes]
        for group in range(groups):
            lower = group * LEAF
            rows = pl.ds(pl.multiple_of(base + lower, LEAF), LEAF)
            left = ref[:, lanes]
            inside = (lanes_left >= lower) & (lanes_left < lower + LEAF)
            high, middle, low = split(jnp.where(inside, left, 0.0))
            twice = high + pltpu.roll(middle, LEAF, 1)
            packed = twice + pltpu.roll(twice, 2 * LEAF, 1)
            packed = packed + pltpu.roll(high, 4 * LEAF, 1) + pltpu.roll(low, 5 * LEAF, 1)
            left_ref[...] = packed.astype(jnp.bfloat16)
            ref[:, lanes] = jnp.where(inside, 0.0, left)
            columns = [
                jnp.broadcast_to(tile[:, lower + k : lower + k + 1], (LEAF, LANES))
                for k in range(LEAF)
            ]
            here = lanes_wide - (base + lower)
            unit = jnp.where(here == rows_wide, 1.0, 0.0)
            wide = jnp.where((here >= 0) & (here < LEAF), unit, wide)
            parts = [wide[:, part * LANES : (part + 1) * LANES] for part in range(blocks)]
            for k in range(LEAF):
                pivot = columns[k][k : k + 1, :]
                inverted = 1.0 / pivot
                factor = jnp.where(rows_leaf == k, pivot - 1.0, columns[k])
                for later in range(k + 1, LEAF):
                    row = columns[later][k : k + 1, :] * inverted
                    columns[later] = columns[later] - factor * row
                parts = [part - factor * (part[k : k + 1, :] * inverted) for part in parts]
            done = jnp.concatenate(parts, axis=1)
            high, middle, low = [part.astype(jnp.bfloat16) for part in split(done)]
            pieces = [nothing] * groups
            for place, piece in enumerate((high, high, middle, middle, low, high)):
                pieces[(group + place) % groups] = piece
            right = jnp.concatenate(pieces, axis=0)
            if group < groups - 1:
                after = pl.ds(pl.multiple_of(base + lower + LEAF, LEAF), LEAF)
                change = jnp.dot(left_ref[after, :], right, preferred_element_type=jnp.float32)
                wide = ref[after, :] - change
                chosen = change[:, :LANES]
                for part in range(1, blocks):
                    chosen = jnp.where(
                        number == part, change[:, part * LANES : (part + 1) * LANES], chosen
                    )
                tile = ref[after, lanes] - chosen
            ref[...] = ref[...] - jnp.dot(
                left_ref[...], right, preferred_element_type=jnp.float32
            )
            ref[rows, :] = done
        return 0

    lax.fori_loop(0, blocks, block, 0)


def raw_dot(left, right, contract=(1, 0)):
    dims = (((contract[0],), (contract[1],)), ((), ()))
    return lax.dot_general(left, right, dims, preferred_element_type=jnp.float32)


def joined(terms, contract=(1, 0)):
    left = jnp.concatenate([term[0] for term in terms], axis=contract[0])
    right = jnp.concatenate([term[1] for term in terms], axis=contract[1])
    return raw_dot(left, right, contract)


def halves(value):
    return [part.astype(jnp.bfloat16) for part in split(value)]


def fetch(source, target, semaphore):
    copy = pltpu.make_async_copy(source, target, semaphore)
    copy.start()
    copy.wait()


def first_kernel(
    flags, own, sibling, lefts_out, ng_out, t_out, n_ref, a_ref, left_ref, semaphore, own_ref, more
):
    order = a_ref.shape[0]
    head = pl.ds(0, order)
    tail = pl.ds(order, own.shape[0] - order)

    fetch(own, own_ref, semaphore)

    @pl.when(flags[0] == 0)
    def _():
        fetch(own_ref, lefts_out, semaphore)

    @pl.when(flags[0] != 0)
    def _():
        @pl.when(flags[1] != 0)
        def _():
            n_ref[...] = own_ref[head, :]
            fetch(sibling, a_ref, semaphore)

        @pl.when(flags[1] == 0)
        def _():
            fetch(sibling, n_ref, semaphore)
            a_ref[...] = own_ref[head, :]

        invert(n_ref, left_ref)
        a10 = a_ref[...].astype(jnp.bfloat16)
        g = joined([(part, a10) for part in reversed(halves(n_ref[...]))])
        a_ref[...] = joined([(a10, part) for part in reversed(halves(g))], (0, 0))
        n_ref[...] = jnp.where(flags[1] != 0, g, n_ref[...])
        copies = [
            pltpu.make_async_copy(source, target, more.at[i])
            for i, (source, target) in enumerate(
                [
                    (n_ref, ng_out),
                    (a_ref, t_out),
                    (n_ref, lefts_out.at[head]),
                    (own_ref.at[tail], lefts_out.at[tail]),
                ]
            )
        ]
        for copy in copies:
            copy.start()
        for copy in copies:
            copy.wait()


def second_kernel(flags, t, a00, s_out, s_ref, a_ref, left_ref, semaphore):
    half = s_out.shape[0]

    @pl.when(flags[0] != 0)
    def _():
        fetch(t, a_ref, semaphore)
        fetch(a00, s_ref, semaphore)
        s_ref[...] = s_ref[...] - a_ref[...]
        invert(s_ref, left_ref)

        @pl.when(flags[1] != 0)
        def _():
            fetch(s_ref.at[pl.ds(half, half)], s_out, semaphore)

        @pl.when(flags[1] == 0)
        def _():
            fetch(s_ref.at[pl.ds(0, half)], s_out, semaphore)


def pivot_call(kernel, flags, left, right, outs, more=()):
    order = right.shape[0]
    anywhere = pl.BlockSpec(memory_space=pl.ANY)
    return pl.pallas_call(
        kernel,
        out_shape=[jax.ShapeDtypeStruct(shape, jnp.float32) for shape in outs],
        in_specs=[pl.BlockSpec(memory_space=pltpu.SMEM), anywhere, anywhere],
        out_specs=[anywhere] * len(outs),
        scratch_shapes=[
            pltpu.VMEM((order, order), jnp.float32),
            pltpu.VMEM((order, order), jnp.float32),
            pltpu.VMEM((order, LANES), jnp.bfloat16),
            pltpu.SemaphoreType.DMA,
            *more,
        ],
    )(flags, left, right)


def transfer(cases, semaphores, begin, place=0):
    for condition, copies in cases:
        @pl.when(condition)
        def _(copies=copies, place=place):
            for i, (source, target) in enumerate(copies):
                copy = pltpu.make_async_copy(source, target, semaphores.at[place + i])
                if begin:
                    copy.start()
                else:
                    copy.wait()

        place += len(copies)
    return place


def pack_kernel(flags, lefts, sibling, near, out, held, semaphores):
    order = out.shape[0] // 2
    at = pl.ds(pl.multiple_of(flags[1] * order, order), order)
    head, tail = pl.ds(0, order), pl.ds(order, order)
    far, odd = flags[0] != 0, flags[2] != 0
    cases = [
        (jnp.logical_not(far), [(near, held)]),
        (far & odd, [(sibling.at[at], held.at[head]), (lefts.at[at], held.at[tail])]),
        (
            far & jnp.logical_not(odd),
            [(lefts.at[at], held.at[head]), (sibling.at[at], held.at[tail])],
        ),
    ]
    transfer(cases, semaphores, True)
    transfer(cases, semaphores, False)
    fetch(held, out, semaphores.at[0])


def pack(flags, lefts, sibling, near):
    anywhere = pl.BlockSpec(memory_space=pl.ANY)
    return pl.pallas_call(
        pack_kernel,
        out_shape=jax.ShapeDtypeStruct(near.shape, jnp.float32),
        in_specs=[pl.BlockSpec(memory_space=pltpu.SMEM)] + [anywhere] * 3,
        out_specs=anywhere,
        scratch_shapes=[pltpu.VMEM(near.shape, jnp.float32), pltpu.SemaphoreType.DMA((5,))],
        name="pack",
    )(flags, lefts, sibling, near)


FIRST, SECOND, TOP, BOTTOM, NEAR, FAR, PACKED, LATER = range(8)


PRODUCTS = ((0, 2), (2, 0), (1, 1), (0, 1), (1, 0), (0, 0))


def finish_kernel(
    flags, mine, lefts, sibling, across, near, far, packed, ng, ng_sibling, s_mine, s_other, out,
    mine_ref, left0_ref, left1_ref, n_ref, g_ref, r_ref, s_ref, semaphores
):
    order = n_ref.shape[0]
    half = order // 2
    kind, odd, in_root, pivotal = flags[0], flags[1] != 0, flags[2] != 0, flags[3] != 0
    in_top = flags[4] != 0
    head, tail = pl.ds(0, order), pl.ds(order, order)
    upper, lower = s_ref.at[pl.ds(0, half)], s_ref.at[pl.ds(half, half)]
    even = jnp.logical_not(odd)
    elsewhere = jnp.logical_not(in_root)
    first = [
        (kind == TOP, [(mine.at[head], r_ref.at[head]), (across, r_ref.at[tail])]),
        (kind == BOTTOM, [(across, r_ref.at[head]), (mine.at[head], r_ref.at[tail])]),
        (kind == NEAR, [(near, r_ref)]),
        ((kind == FAR) | (kind == LATER), [(far, r_ref)]),
        (kind == PACKED, [(packed, r_ref)]),
        (elsewhere & even, [(ng, n_ref), (ng_sibling, g_ref)]),
        (elsewhere & odd, [(ng_sibling, n_ref), (ng, g_ref)]),
        (in_root & even, [(lefts.at[head], n_ref), (sibling.at[head], g_ref)]),
        (in_root & odd, [(sibling.at[head], n_ref), (lefts.at[head], g_ref)]),
        (even, [(s_mine, upper), (s_other, lower)]),
        (odd, [(s_other, upper), (s_mine, lower)]),
    ]
    second = [
        (even, [(lefts, left0_ref), (sibling, left1_ref)]),
        (odd, [(sibling, left0_ref), (lefts, left1_ref)]),
        (kind >= 0, [(mine, mine_ref)]),
    ]
    place = transfer(first, semaphores, True)
    transfer(second, semaphores, True, place)
    transfer(first, semaphores, False)

    @pl.when((kind == FAR) | (kind == PACKED))
    def _():
        r_ref[head, :] = r_ref[head, :].T
        r_ref[tail, :] = r_ref[tail, :].T

    @pl.when((kind == FIRST) | (kind == SECOND))
    def _():
        rows = lax.broadcasted_iota(jnp.int32, (order, order), 0)
        lanes = lax.broadcasted_iota(jnp.int32, (order, order), 1)
        unit = jnp.where(rows == lanes, 1.0, 0.0)
        r_ref[head, :] = jnp.where(kind == FIRST, unit, 0.0)
        r_ref[tail, :] = jnp.where(kind == FIRST, 0.0, unit)

    r1 = r_ref[tail, :].astype(jnp.bfloat16)
    g = halves(g_ref[...])
    n = halves(n_ref[...])
    s = halves(s_ref[...])
    y = halves(r_ref[head, :] - joined([(part, r1) for part in reversed(g)], (0, 0)))
    w0 = joined([(s[i], y[j]) for i, j in PRODUCTS])
    w = halves(w0)
    w1 = joined([(part, r1) for part in reversed(n)])
    w1 = w1 - joined([(g[i], w[j]) for i, j in PRODUCTS])
    v = halves(w1)
    transfer(second, semaphores, False, place)
    left0 = left0_ref[...].astype(jnp.bfloat16)
    left1 = left1_ref[...].astype(jnp.bfloat16)
    change = joined([(left0, w[i]) for i in (2, 1, 0)] + [(left1, v[i]) for i in (2, 1, 0)])
    mine_ref[...] = jnp.where(pivotal, 0.0, mine_ref[...]) - change

    @pl.when(in_top)
    def _():
        mine_ref[head, :] = w0

    @pl.when(in_root)
    def _():
        mine_ref[head, :] = w1

    count = order // LANES
    for part in range(count):
        where = pl.ds(part, mine_ref.shape[0], stride=count)
        out[where, :] = mine_ref[:, part * LANES : (part + 1) * LANES]


def finish(flags, *arrays):
    mine = arrays[0]
    order = mine.shape[1]
    anywhere = pl.BlockSpec(memory_space=pl.ANY)
    square, whole = pltpu.VMEM((order, order), jnp.float32), pltpu.VMEM(mine.shape, jnp.float32)
    linear = (mine.shape[0] * order // LANES, LANES)
    return pl.pallas_call(
        finish_kernel,
        out_shape=jax.ShapeDtypeStruct(linear, jnp.float32),
        in_specs=[pl.BlockSpec(memory_space=pltpu.SMEM)] + [anywhere] * len(arrays),
        out_specs=pl.BlockSpec(memory_space=pltpu.VMEM),
        scratch_shapes=[whole, whole, whole, square, square]
        + [pltpu.VMEM((2 * order, order), jnp.float32), square, pltpu.SemaphoreType.DMA((32,))],
        name="finish",
    )(flags, *arrays)


def sweep(gram):
    row_count = lax.axis_size("row")
    col_count = lax.axis_size("col")
    here_row = lax.axis_index("row")
    here_col = lax.axis_index("col")
    breadth = gram.shape[2]
    mine = gram.astype(jnp.float32).reshape(gram.shape[0] * breadth, breadth)
    first = mine[:breadth]
    odd = here_col % 2 == 1
    pair = here_col // 2
    steps = (col_count // 2).bit_length() - 1
    root = 1

    def send(value, pairs):
        lines = [(a[0] * col_count + a[1], b[0] * col_count + b[1]) for a, b in pairs]
        return lax.ppermute(value, ("row", "col"), lines)

    def swap(value):
        pairs = [((r, c), (r, c ^ 1)) for r in range(row_count) for c in range(col_count)]
        return send(value, pairs)

    def after(value, *others):
        return lax.optimization_barrier((value,) + others)[0]

    def along_row(value, which, *earlier):
        held = value
        for step in range(steps):
            pairs = []
            takes = jnp.zeros((), jnp.bool_)
            for parity in range(2):
                done = list(range(step)) if parity == 0 else list(range(steps - step, steps))
                bit = step if parity == 0 else steps - 1 - step
                targets = []
                for number in range(col_count // 2):
                    if all(number >> b & 1 == 0 for b in range(steps) if b not in done):
                        target = number | 1 << bit
                        targets.append(target)
                        for r in which:
                            pairs.append(((r, 2 * number + parity), (r, 2 * target + parity)))
                for target in targets:
                    takes = takes | (here_col == 2 * target + parity)
            got = send(held, pairs)
            if step == 0 and earlier:
                got = after(got, *earlier)
            held = jnp.where(takes, got, held)
        return held

    def along_column(value, columns, *earlier):
        result = after(value, *earlier) if earlier else value
        for chain in (range(root, 0, -1), range(root, row_count - 1)):
            held = value
            for r in chain:
                upward = chain.step < 0
                target = r - 1 if upward else r + 1
                held = send(held, [((r, c), (target, c)) for c in columns])
                result = jnp.where(here_row == target, held, result)
        return result

    others = range(2, col_count)
    sibling = swap(first)
    across = send(
        jnp.where((here_col == 1) & (here_row == 0), sibling, first),
        [((0, c), (1, c)) for c in range(col_count)] + [((1, c), (0, c)) for c in others],
    )

    at_root = (here_row == root) & (pair == 0)
    flags = jnp.stack([at_root.astype(jnp.int32), odd.astype(jnp.int32)])
    half = breadth // 2
    square = (breadth, breadth)
    lefts, ng, t = pivot_call(
        first_kernel,
        flags,
        mine,
        sibling,
        [mine.shape, square, square],
        [pltpu.VMEM(mine.shape, jnp.float32), pltpu.SemaphoreType.DMA((4,))],
    )
    (s_half,) = pivot_call(second_kernel, flags, t, across, [(half, breadth)])

    lefts = along_row(lefts, range(row_count))
    lefts_sibling = swap(lefts)

    own_row = here_col % row_count
    slot = here_col // row_count
    near = [c for c in others if c % row_count < 2]
    far = [c for c in others if c % row_count >= 2]
    is_far = (own_row >= 2) & (here_col >= 2)
    down_near = jnp.concatenate([across, first], axis=0)
    passed = send(down_near, [((1, c), (2, c)) for c in near])
    pack_flags = jnp.stack(
        [(is_far & (here_row == own_row)).astype(jnp.int32), slot, odd.astype(jnp.int32)]
    )
    packed = pack(pack_flags, lefts, lefts_sibling, passed)
    if row_count == 4:
        pairs = [((2, c), (3, c)) for c in near]
        pairs += [((c % row_count, c), (5 - c % row_count, c)) for c in far]
        later = send(packed, pairs)
    else:
        held = passed
        for r in range(2, row_count - 1):
            passed = send(passed, [((r, c), (r + 1, c)) for c in near])
            held = jnp.where(here_row == r + 1, passed, held)
        passed = held
        later = packed
        for sign in (1, -1):
            moving = packed
            for step in range(row_count - 3):
                pairs = []
                for c in far:
                    source = c % row_count + sign * step
                    if 2 <= source < row_count and 2 <= source + sign < row_count:
                        pairs.append(((source, c), (source + sign, c)))
                moving = send(moving, pairs)
                later = jnp.where(here_row == own_row + sign * (step + 1), moving, later)
    kind = jnp.where(here_row == 2, NEAR, LATER if row_count == 4 else NEAR)
    kind = jnp.where(is_far & (here_row >= 2), jnp.where(here_row == own_row, PACKED, FAR), kind)
    kind = jnp.where(here_row == 0, TOP, jnp.where(here_row == 1, BOTTOM, kind))
    kind = jnp.where(here_col == 0, FIRST, jnp.where(here_col == 1, SECOND, kind))

    ng = along_column(ng, range(2))
    chained = ng
    ng = along_row(ng, [r for r in range(row_count) if r != root], packed)
    ng_sibling = swap(ng)
    pivotal = here_col < 2
    s_root = along_row(s_half, [root])
    s_half = along_column(s_half, range(2), chained)
    s_half = along_row(s_half, [r for r in range(row_count) if r != root])
    s_half = jnp.where(here_row == root, s_root, s_half)
    s_sibling = swap(s_half)
    tests = [kind, odd, here_row == root, pivotal, here_row == 0]
    finish_flags = jnp.stack([test.astype(jnp.int32) for test in tests])
    out = finish(
        finish_flags,
        mine, lefts, lefts_sibling, across, passed, later, packed, ng, ng_sibling,
        s_half, s_sibling,
    )
    return out.reshape(gram.shape)


def solution(mesh):
    placed = (P(None, "row", None, None, "col", None),)
    return jax.shard_map(
        sweep,
        mesh=mesh,
        in_specs=placed,
        out_specs=P(None, "row", None, None, "col", None),
        check_vma=False,
    )
```

```python
import jax
import jax.numpy as jnp
from jax import lax
from jax.experimental import pallas as pl
from jax.experimental.pallas import tpu as pltpu
from jax.sharding import PartitionSpec as P


LEAF = 16
LANES = 128


def split(value):
    high = value.astype(jnp.bfloat16).astype(jnp.float32)
    rest = value - high
    middle = rest.astype(jnp.bfloat16).astype(jnp.float32)
    return high, middle, (rest - middle).astype(jnp.bfloat16).astype(jnp.float32)


def invert(ref, left_ref):
    order = ref.shape[0]
    blocks = order // LANES
    groups = LANES // LEAF
    rows_leaf = lax.broadcasted_iota(jnp.int32, (LEAF, LANES), 0)
    rows_wide = lax.broadcasted_iota(jnp.int32, (LEAF, order), 0)
    lanes_wide = lax.broadcasted_iota(jnp.int32, (LEAF, order), 1)
    lanes_left = lax.broadcasted_iota(jnp.int32, (order, LANES), 1)
    nothing = jnp.zeros((LEAF, order), jnp.bfloat16)

    def block(number, _):
        base = pl.multiple_of(number * LANES, LANES)
        lanes = pl.ds(base, LANES)
        wide = ref[pl.ds(base, LEAF), :]
        tile = ref[pl.ds(base, LEAF), lanes]
        for group in range(groups):
            lower = group * LEAF
            rows = pl.ds(pl.multiple_of(base + lower, LEAF), LEAF)
            left = ref[:, lanes]
            inside = (lanes_left >= lower) & (lanes_left < lower + LEAF)
            high, middle, low = split(jnp.where(inside, left, 0.0))
            packed = high + pltpu.roll(middle, LEAF, 1)
            packed = packed + (pltpu.roll(high, 2 * LEAF, 1) + pltpu.roll(middle, 3 * LEAF, 1))
            packed = packed + (pltpu.roll(high, 4 * LEAF, 1) + pltpu.roll(low, 5 * LEAF, 1))
            left_ref[...] = packed.astype(jnp.bfloat16)
            ref[:, lanes] = jnp.where(inside, 0.0, left)
            columns = [
                jnp.broadcast_to(tile[:, lower + k : lower + k + 1], (LEAF, LANES))
                for k in range(LEAF)
            ]
            here = lanes_wide - (base + lower)
            unit = jnp.where(here == rows_wide, 1.0, 0.0)
            wide = jnp.where((here >= 0) & (here < LEAF), unit, wide)
            parts = [wide[:, part * LANES : (part + 1) * LANES] for part in range(blocks)]
            for k in range(LEAF):
                pivot = columns[k][k : k + 1, :]
                inverted = 1.0 / pivot
                factor = jnp.where(rows_leaf == k, pivot - 1.0, columns[k])
                for later in range(k + 1, LEAF):
                    row = columns[later][k : k + 1, :] * inverted
                    columns[later] = columns[later] - factor * row
                parts = [part - factor * (part[k : k + 1, :] * inverted) for part in parts]
            done = jnp.concatenate(parts, axis=1)
            high, middle, low = [part.astype(jnp.bfloat16) for part in split(done)]
            pieces = [nothing] * groups
            for place, piece in enumerate((high, high, middle, middle, low, high)):
                pieces[(group + place) % groups] = piece
            right = jnp.concatenate(pieces, axis=0)
            if group < groups - 1:
                after = pl.ds(pl.multiple_of(base + lower + LEAF, LEAF), LEAF)
                change = jnp.dot(left_ref[after, :], right, preferred_element_type=jnp.float32)
                wide = ref[after, :] - change
                chosen = change[:, :LANES]
                for part in range(1, blocks):
                    chosen = jnp.where(
                        number == part, change[:, part * LANES : (part + 1) * LANES], chosen
                    )
                tile = ref[after, lanes] - chosen
            ref[...] = ref[...] - jnp.dot(
                left_ref[...], right, preferred_element_type=jnp.float32
            )
            ref[rows, :] = done
        return 0

    lax.fori_loop(0, blocks, block, 0)


def raw_dot(left, right, contract=(1, 0)):
    dims = (((contract[0],), (contract[1],)), ((), ()))
    return lax.dot_general(left, right, dims, preferred_element_type=jnp.float32)


def joined(terms, contract=(1, 0)):
    left = jnp.concatenate([term[0] for term in terms], axis=contract[0])
    right = jnp.concatenate([term[1] for term in terms], axis=contract[1])
    return raw_dot(left, right, contract)


def pieces(value):
    high = value.astype(jnp.bfloat16)
    return high, (value - high.astype(jnp.float32)).astype(jnp.bfloat16)


def halves(value):
    return [part.astype(jnp.bfloat16) for part in split(value)]


def fetch(source, target, semaphore):
    copy = pltpu.make_async_copy(source, target, semaphore)
    copy.start()
    copy.wait()


def first_kernel(
    flags, own, sibling, lefts_out, ng_out, t_out, n_ref, a_ref, left_ref, semaphore, own_ref, more
):
    order = a_ref.shape[0]
    head = pl.ds(0, order)
    tail = pl.ds(order, own.shape[0] - order)

    fetch(own, own_ref, semaphore)

    @pl.when(flags[0] == 0)
    def _():
        fetch(own_ref, lefts_out, semaphore)

    @pl.when(flags[0] != 0)
    def _():
        @pl.when(flags[1] != 0)
        def _():
            n_ref[...] = own_ref[head, :]
            fetch(sibling, a_ref, semaphore)

        @pl.when(flags[1] == 0)
        def _():
            fetch(sibling, n_ref, semaphore)
            a_ref[...] = own_ref[head, :]

        invert(n_ref, left_ref)
        a10 = a_ref[...].astype(jnp.bfloat16)
        g = joined([(part, a10) for part in reversed(halves(n_ref[...]))])
        a_ref[...] = joined([(a10, part) for part in reversed(halves(g))], (0, 0))
        n_ref[...] = jnp.where(flags[1] != 0, g, n_ref[...])
        copies = [
            pltpu.make_async_copy(source, target, more.at[i])
            for i, (source, target) in enumerate(
                [
                    (n_ref, ng_out),
                    (a_ref, t_out),
                    (n_ref, lefts_out.at[head]),
                    (own_ref.at[tail], lefts_out.at[tail]),
                ]
            )
        ]
        for copy in copies:
            copy.start()
        for copy in copies:
            copy.wait()


def second_kernel(
    flags, t, across, first, s_out, near_out, s_ref, a_ref, left_ref, semaphore
):
    order = a_ref.shape[0]
    half = s_out.shape[0]

    @pl.when(flags[2] != 0)
    def _():
        fetch(across, s_ref, semaphore)
        fetch(first, a_ref, semaphore)
        fetch(s_ref, near_out.at[pl.ds(0, order)], semaphore)
        fetch(a_ref, near_out.at[pl.ds(order, order)], semaphore)

    @pl.when(flags[0] != 0)
    def _():
        fetch(t, a_ref, semaphore)
        fetch(across, s_ref, semaphore)
        s_ref[...] = s_ref[...] - a_ref[...]
        invert(s_ref, left_ref)

        @pl.when(flags[1] != 0)
        def _():
            fetch(s_ref.at[pl.ds(half, half)], s_out, semaphore)

        @pl.when(flags[1] == 0)
        def _():
            fetch(s_ref.at[pl.ds(0, half)], s_out, semaphore)


def pivot_call(kernel, flags, arrays, outs, more=()):
    order = arrays[1].shape[0]
    anywhere = pl.BlockSpec(memory_space=pl.ANY)
    return pl.pallas_call(
        kernel,
        out_shape=[jax.ShapeDtypeStruct(shape, jnp.float32) for shape in outs],
        in_specs=[pl.BlockSpec(memory_space=pltpu.SMEM)] + [anywhere] * len(arrays),
        out_specs=[anywhere] * len(outs),
        scratch_shapes=[
            pltpu.VMEM((order, order), jnp.float32),
            pltpu.VMEM((order, order), jnp.float32),
            pltpu.VMEM((order, LANES), jnp.bfloat16),
            pltpu.SemaphoreType.DMA,
            *more,
        ],
    )(flags, *arrays)


def transfer(cases, semaphores, begin, place=0):
    for condition, copies in cases:
        @pl.when(condition)
        def _(copies=copies, place=place):
            for i, (source, target) in enumerate(copies):
                copy = pltpu.make_async_copy(source, target, semaphores.at[place + i])
                if begin:
                    copy.start()
                else:
                    copy.wait()

        place += len(copies)
    return place


def pack_kernel(flags, lefts, sibling, near, out, held, semaphores):
    order = out.shape[0] // 2
    at = pl.ds(pl.multiple_of(flags[1] * order, order), order)
    head, tail = pl.ds(0, order), pl.ds(order, order)
    far, odd, close = flags[0] != 0, flags[2] != 0, flags[3] != 0
    cases = [
        (close, [(near, held)]),
        (far & odd, [(sibling.at[at], held.at[head]), (lefts.at[at], held.at[tail])]),
        (
            far & jnp.logical_not(odd),
            [(lefts.at[at], held.at[head]), (sibling.at[at], held.at[tail])],
        ),
    ]
    transfer(cases, semaphores, True)
    transfer(cases, semaphores, False)

    @pl.when(far | close)
    def _():
        fetch(held, out, semaphores.at[0])


def pack(flags, lefts, sibling, near):
    anywhere = pl.BlockSpec(memory_space=pl.ANY)
    return pl.pallas_call(
        pack_kernel,
        out_shape=jax.ShapeDtypeStruct(near.shape, jnp.float32),
        in_specs=[pl.BlockSpec(memory_space=pltpu.SMEM)] + [anywhere] * 3,
        out_specs=anywhere,
        scratch_shapes=[pltpu.VMEM(near.shape, jnp.float32), pltpu.SemaphoreType.DMA((5,))],
        name="pack",
    )(flags, lefts, sibling, near)


FIRST, SECOND, TOP, BOTTOM, NEAR, FAR, PACKED, LATER = range(8)


PRODUCTS = ((0, 1), (1, 0), (0, 0))


def finish_kernel(
    flags, mine, lefts, sibling, across, near, far, packed, ng, ng_sibling, s_mine, s_other, out,
    mine_ref, left0_ref, left1_ref, n_ref, g_ref, r_ref, s_ref, semaphores
):
    order = n_ref.shape[0]
    half = order // 2
    kind, odd, in_root, pivotal = flags[0], flags[1] != 0, flags[2] != 0, flags[3] != 0
    in_top = flags[4] != 0
    head, tail = pl.ds(0, order), pl.ds(order, order)
    upper, lower = s_ref.at[pl.ds(0, half)], s_ref.at[pl.ds(half, half)]
    even = jnp.logical_not(odd)
    elsewhere = jnp.logical_not(in_root)
    first = [
        (kind == TOP, [(mine.at[head], r_ref.at[head]), (across, r_ref.at[tail])]),
        (kind == BOTTOM, [(across, r_ref.at[head]), (mine.at[head], r_ref.at[tail])]),
        (kind == NEAR, [(near, r_ref)]),
        ((kind == FAR) | (kind == LATER), [(far, r_ref)]),
        (kind == PACKED, [(packed, r_ref)]),
        (elsewhere & even, [(ng, n_ref), (ng_sibling, g_ref)]),
        (elsewhere & odd, [(ng_sibling, n_ref), (ng, g_ref)]),
        (in_root & even, [(lefts.at[head], n_ref), (sibling.at[head], g_ref)]),
        (in_root & odd, [(sibling.at[head], n_ref), (lefts.at[head], g_ref)]),
        (even, [(s_mine, upper), (s_other, lower)]),
        (odd, [(s_other, upper), (s_mine, lower)]),
    ]
    second = [
        (even, [(lefts, left0_ref), (sibling, left1_ref)]),
        (odd, [(sibling, left0_ref), (lefts, left1_ref)]),
        (kind >= 0, [(mine, mine_ref)]),
    ]
    place = transfer(first, semaphores, True)
    transfer(second, semaphores, True, place)
    transfer(first, semaphores, False)

    @pl.when((kind == FAR) | (kind == PACKED))
    def _():
        r_ref[head, :] = r_ref[head, :].T
        r_ref[tail, :] = r_ref[tail, :].T

    @pl.when((kind == FIRST) | (kind == SECOND))
    def _():
        rows = lax.broadcasted_iota(jnp.int32, (order, order), 0)
        lanes = lax.broadcasted_iota(jnp.int32, (order, order), 1)
        unit = jnp.where(rows == lanes, 1.0, 0.0)
        r_ref[head, :] = jnp.where(kind == FIRST, unit, 0.0)
        r_ref[tail, :] = jnp.where(kind == FIRST, 0.0, unit)

    r1 = r_ref[tail, :].astype(jnp.bfloat16)
    g, n, s = [pieces(ref[...]) for ref in (g_ref, n_ref, s_ref)]
    y = pieces(r_ref[head, :] - joined([(part, r1) for part in reversed(g)], (0, 0)))
    w0 = joined([(s[i], y[j]) for i, j in PRODUCTS])
    w = pieces(w0)
    w1 = joined([(part, r1) for part in reversed(n)])
    w1 = w1 - joined([(g[i], w[j]) for i, j in PRODUCTS])
    v = pieces(w1)
    transfer(second, semaphores, False, place)
    left0 = left0_ref[...].astype(jnp.bfloat16)
    left1 = left1_ref[...].astype(jnp.bfloat16)
    sides = [jnp.concatenate(parts, axis=1) for parts in (w, v)]
    both = joined([(left0, sides[0]), (left1, sides[1])])
    change = both[:, order:] + both[:, :order]
    mine_ref[...] = jnp.where(pivotal, 0.0, mine_ref[...]) - change

    @pl.when(in_top)
    def _():
        mine_ref[head, :] = w0

    @pl.when(in_root)
    def _():
        mine_ref[head, :] = w1

    count = order // LANES
    for part in range(count):
        where = pl.ds(part, mine_ref.shape[0], stride=count)
        out[where, :] = mine_ref[:, part * LANES : (part + 1) * LANES]


def finish(flags, *arrays):
    mine = arrays[0]
    order = mine.shape[1]
    anywhere = pl.BlockSpec(memory_space=pl.ANY)
    square, whole = pltpu.VMEM((order, order), jnp.float32), pltpu.VMEM(mine.shape, jnp.float32)
    linear = (mine.shape[0] * order // LANES, LANES)
    return pl.pallas_call(
        finish_kernel,
        out_shape=jax.ShapeDtypeStruct(linear, jnp.float32),
        in_specs=[pl.BlockSpec(memory_space=pltpu.SMEM)] + [anywhere] * len(arrays),
        out_specs=pl.BlockSpec(memory_space=pltpu.VMEM),
        scratch_shapes=[whole, whole, whole, square, square]
        + [pltpu.VMEM((2 * order, order), jnp.float32), square, pltpu.SemaphoreType.DMA((32,))],
        name="finish",
    )(flags, *arrays)


def sweep(gram):
    row_count = lax.axis_size("row")
    col_count = lax.axis_size("col")
    here_row = lax.axis_index("row")
    here_col = lax.axis_index("col")
    breadth = gram.shape[2]
    mine = gram.astype(jnp.float32).reshape(gram.shape[0] * breadth, breadth)
    first = mine[:breadth]
    odd = here_col % 2 == 1
    pair = here_col // 2
    steps = (col_count // 2).bit_length() - 1
    root = 1

    def send(value, pairs):
        lines = [(a[0] * col_count + a[1], b[0] * col_count + b[1]) for a, b in pairs]
        return lax.ppermute(value, ("row", "col"), lines)

    def swap(value):
        pairs = [((r, c), (r, c ^ 1)) for r in range(row_count) for c in range(col_count)]
        return send(value, pairs)

    def after(value, *others):
        return lax.optimization_barrier((value,) + others)[0]

    def along_row(value, which, *earlier):
        held = value
        for step in range(steps):
            pairs = []
            takes = jnp.zeros((), jnp.bool_)
            for parity in range(2):
                done = list(range(step)) if parity == 0 else list(range(steps - step, steps))
                bit = step if parity == 0 else steps - 1 - step
                targets = []
                for number in range(col_count // 2):
                    if all(number >> b & 1 == 0 for b in range(steps) if b not in done):
                        target = number | 1 << bit
                        targets.append(target)
                        for r in which:
                            pairs.append(((r, 2 * number + parity), (r, 2 * target + parity)))
                for target in targets:
                    takes = takes | (here_col == 2 * target + parity)
            got = send(held, pairs)
            if step == 0 and earlier:
                got = after(got, *earlier)
            held = jnp.where(takes, got, held)
        return held

    def along_column(value, columns, *earlier):
        result = after(value, *earlier) if earlier else value
        for chain in (range(root, 0, -1), range(root, row_count - 1)):
            held = value
            for r in chain:
                upward = chain.step < 0
                target = r - 1 if upward else r + 1
                held = send(held, [((r, c), (target, c)) for c in columns])
                result = jnp.where(here_row == target, held, result)
        return result

    others = range(2, col_count)
    sibling = swap(first)
    across = send(
        jnp.where((here_col == 1) & (here_row == 0), sibling, first),
        [((0, c), (1, c)) for c in range(col_count)] + [((1, c), (0, c)) for c in others],
    )

    at_root = (here_row == root) & (pair == 0)
    to_near = (here_row == 1) & (here_col >= 2) & (here_col % row_count < 2)
    flags = jnp.stack([test.astype(jnp.int32) for test in (at_root, odd, to_near)])
    half = breadth // 2
    square = (breadth, breadth)
    lefts, ng, t = pivot_call(
        first_kernel,
        flags,
        [mine, sibling],
        [mine.shape, square, square],
        [pltpu.VMEM(mine.shape, jnp.float32), pltpu.SemaphoreType.DMA((4,))],
    )
    s_half, down_near = pivot_call(
        second_kernel, flags, [t, across, first], [(half, breadth), mine.shape]
    )

    lefts = along_row(lefts, range(row_count))
    lefts_sibling = swap(lefts)

    own_row = here_col % row_count
    slot = here_col // row_count
    near = [c for c in others if c % row_count < 2]
    far = [c for c in others if c % row_count >= 2]
    is_far = (own_row >= 2) & (here_col >= 2)
    passed = send(down_near, [((1, c), (2, c)) for c in near])
    is_close = (here_row == 2) & (own_row < 2) & (here_col >= 2)
    tests = [is_far & (here_row == own_row), slot, odd, is_close]
    pack_flags = jnp.stack([test.astype(jnp.int32) for test in tests])
    packed = pack(pack_flags, lefts, lefts_sibling, passed)
    if row_count == 4:
        pairs = [((2, c), (3, c)) for c in near]
        pairs += [((c % row_count, c), (5 - c % row_count, c)) for c in far]
        later = send(packed, pairs)
    else:
        held = passed
        for r in range(2, row_count - 1):
            passed = send(passed, [((r, c), (r + 1, c)) for c in near])
            held = jnp.where(here_row == r + 1, passed, held)
        passed = held
        later = packed
        for sign in (1, -1):
            moving = packed
            for step in range(row_count - 3):
                pairs = []
                for c in far:
                    source = c % row_count + sign * step
                    if 2 <= source < row_count and 2 <= source + sign < row_count:
                        pairs.append(((source, c), (source + sign, c)))
                moving = send(moving, pairs)
                later = jnp.where(here_row == own_row + sign * (step + 1), moving, later)
    kind = jnp.where(here_row == 2, NEAR, LATER if row_count == 4 else NEAR)
    kind = jnp.where(is_far & (here_row >= 2), jnp.where(here_row == own_row, PACKED, FAR), kind)
    kind = jnp.where(here_row == 0, TOP, jnp.where(here_row == 1, BOTTOM, kind))
    kind = jnp.where(here_col == 0, FIRST, jnp.where(here_col == 1, SECOND, kind))

    ng = along_column(ng, range(2))
    chained = ng
    ng = along_row(ng, [r for r in range(row_count) if r != root], packed)
    ng_sibling = swap(ng)
    pivotal = here_col < 2
    s_root = along_row(s_half, [root])
    s_half = along_column(s_half, range(2), chained)
    s_half = along_row(s_half, [r for r in range(row_count) if r != root])
    s_half = jnp.where(here_row == root, s_root, s_half)
    s_sibling = swap(s_half)
    tests = [kind, odd, here_row == root, pivotal, here_row == 0]
    finish_flags = jnp.stack([test.astype(jnp.int32) for test in tests])
    out = finish(
        finish_flags,
        mine, lefts, lefts_sibling, across, passed, later, packed, ng, ng_sibling,
        s_half, s_sibling,
    )
    return out.reshape(gram.shape)


def solution(mesh):
    placed = (P(None, "row", None, None, "col", None),)
    return jax.shard_map(
        sweep,
        mesh=mesh,
        in_specs=placed,
        out_specs=P(None, "row", None, None, "col", None),
        check_vma=False,
    )
```
